32 devices in a mesh: row: 4 (over x, core), col: 8 (over z, y).
Axes of the slice: x: 2, y: 2, z: 4, core: 2. Of those that a mesh axis runs over, the one named last changes fastest.
Arguments:
- w_rec: bfloat16 [2, 4096, 4, 4096], P(None, 'row', None, 'col'), may hold values from -0.09375 to 0.09375
- w_in: bfloat16 [2, 4096, 4, 4096], P(None, 'row', None, 'col'), may hold values from -0.09375 to 0.09375
- gate_pre: float32 [2, 6, 64, 4, 4096], P(None, None, None, None, 'col'), may hold values from -8 to 8, as said below
- cells: float32 [2, 7, 64, 4096], P(None, None, None, 'col'), may hold values from -6 to 6
- layer_in: bfloat16 [2, 6, 64, 4096], P(None, None, None, 'row'), may hold values from -1 to 1
- h_prev: bfloat16 [2, 6, 64, 4096], P(None, None, None, 'row'), may hold values from -1 to 1
- top_grad: float32 [6, 64, 4096], P(None, None, 'col'), may hold values from -40 to 40
Outputs:
- w_rec_grad: bfloat16 [2, 4096, 4, 4096], P(None, 'row', None, 'col')
- w_in_grad: bfloat16 [2, 4096, 4, 4096], P(None, 'row', None, 'col')
- input_grad: float32 [6, 64, 4096], P(None, None, 'col')
The draws below stay inside these ranges and needn't reach their ends.
Inputs may be any that keep to these rules, and one draw needn't show every extreme that they name: `gate_pre`: dimension 3 holds the input, forget, candidate and output gates in that order.
All inputs are finite; a program needn't handle non-finite values.
Results may differ from the reference program's by a relative error of at most 0.0051.
Values sent between devices are 32-bit elements; how exact they have to be, the bound alone decides.
No kernel may reach another device: no remote copies, remote signals or barrier semaphores. Data moves between devices by JAX's collectives and lax.ppermute only.
A program may use at most 128 MiB of HBM per device.

```python
import math
import jax
import jax.numpy as jnp
from jax import lax

WIDTH = 4096
LAYERS = 2
STEPS = 6
BATCH = 64


def draw_gate_pre(key, part):
    first, second = jax.random.split(jax.random.fold_in(key, 11), 2)
    shape = (LAYERS, STEPS, BATCH, 4, WIDTH)
    noise = jax.random.normal(first, shape, jnp.float32)
    offset = jax.random.uniform(second, (LAYERS, 1, 1, 1, WIDTH), jnp.float32, -1.0, 5.0)
    chosen = (jnp.arange(4) == 1).reshape(1, 1, 1, 4, 1)
    values = jnp.where(chosen, offset + 0.7 * noise, 1.5 * noise)
    return jnp.clip(values, -8.0, 8.0)


def draw_top_grad(key, part):
    first, second, third = jax.random.split(jax.random.fold_in(key, 23), 3)
    shape = (STEPS, BATCH, WIDTH)
    phases = jax.random.uniform(first, (2,), jnp.float32, 0.0, 2.0 * math.pi)
    where_unit = jnp.arange(WIDTH).astype(jnp.float32) / WIDTH
    envelope = 1.2 * jnp.sin(2.0 * math.pi * where_unit + phases[0]) + 0.6 * jnp.sin(6.0 * math.pi * where_unit + phases[1])
    factor = 2.0 * jnp.exp(envelope)
    base = jax.random.normal(second, shape, jnp.float32)
    return jnp.clip(base * factor, -40.0, 40.0)


def steps_of(rng, shape, shards, smallest, largest):
    level = 1.0
    for axis_at, blocks in shards:
        heights = jax.random.uniform(jax.random.fold_in(jax.random.fold_in(rng, 6), axis_at), (blocks,), jnp.float32, smallest / len(shards), largest / len(shards))
        level = level * jnp.repeat(jnp.exp(heights), shape[axis_at] // blocks).reshape((-1,) + (1,) * (len(shape) - 1 - axis_at))
    return level


def scatter_about(stream_key, extent, deviation, bound, shards=(), kind=jnp.bfloat16):
    array = deviation * jax.random.normal(stream_key, extent, jnp.float32)
    if shards:
        array = array * steps_of(stream_key, extent, shards, -0.22, 0.18)
    return jnp.clip(array, -bound, bound).astype(kind)


def setup_inputs(seed: int = 0) -> dict:
    streams_of = jax.random.split(jax.random.key(seed), 8)
    return {
        "w_rec": scatter_about(streams_of[0], (LAYERS, WIDTH, 4, WIDTH), WIDTH ** -0.5, 0.09375, ((1, 4), (3, 8))),
        "w_in": scatter_about(streams_of[1], (LAYERS, WIDTH, 4, WIDTH), WIDTH ** -0.5, 0.09375, ((1, 4), (3, 8))),
        "gate_pre": draw_gate_pre(jax.random.fold_in(streams_of[7], 71), 0),
        "cells": scatter_about(streams_of[3], (LAYERS, STEPS + 1, BATCH, WIDTH), 1.0, 6.0, ((3, 8),), jnp.float32),
        "layer_in": jnp.clip(jax.random.uniform(streams_of[4], (LAYERS, STEPS, BATCH, WIDTH), jnp.float32, -1.0, 1.0) * steps_of(streams_of[4], (LAYERS, STEPS, BATCH, WIDTH), ((3, 4),), -0.4, 0.0), -1.0, 1.0).astype(jnp.bfloat16),
        "h_prev": jnp.clip(jax.random.uniform(streams_of[5], (LAYERS, STEPS, BATCH, WIDTH), jnp.float32, -1.0, 1.0) * steps_of(streams_of[5], (LAYERS, STEPS, BATCH, WIDTH), ((3, 4),), -0.4, 0.0), -1.0, 1.0).astype(jnp.bfloat16),
        "top_grad": draw_top_grad(jax.random.fold_in(streams_of[7], 71), 0),
    }


def cell_backward(preact, cell_prev, cell_now, hid_grad, cell_carry):
    in_gate = jax.nn.sigmoid(preact[:, 0])
    forget = jax.nn.sigmoid(preact[:, 1])
    cand_gate = jnp.tanh(preact[:, 2])
    out_gate = jax.nn.sigmoid(preact[:, 3])
    tanh_cell = jnp.tanh(cell_now)
    cell_grad = cell_carry + hid_grad * out_gate * (1.0 - tanh_cell * tanh_cell)
    grad_in = cell_grad * cand_gate * in_gate * (1.0 - in_gate)
    grad_forget = cell_grad * cell_prev * forget * (1.0 - forget)
    grad_cand = cell_grad * in_gate * (1.0 - cand_gate * cand_gate)
    grad_out = hid_grad * tanh_cell * out_gate * (1.0 - out_gate)
    gate_grads = jnp.stack([grad_in, grad_forget, grad_cand, grad_out], axis=1).astype(jnp.bfloat16)
    return (gate_grads, cell_grad * forget)

def reference(w_rec, w_in, gate_pre, cells, layer_in, h_prev, top_grad):
    incoming = top_grad
    rec_grads = [None] * LAYERS
    in_grads = [None] * LAYERS
    sumsq = jnp.zeros((), jnp.float32)
    for layer in range(LAYERS - 1, -1, -1):
        rec_flat = w_rec[layer].reshape(WIDTH, 4 * WIDTH)

        def advance(carry, inputs, rec_flat=rec_flat):
            rec_carry, cell_carry = carry
            preact, cell_prev, cell_now, outside = inputs
            gate_grads, cell_next = cell_backward(preact, cell_prev, cell_now, outside + rec_carry, cell_carry)
            recurrent = jnp.dot(gate_grads.reshape(BATCH, 4 * WIDTH), rec_flat.T, preferred_element_type=jnp.float32)
            return ((recurrent, cell_next), gate_grads)
        zeros = jnp.zeros((BATCH, WIDTH), jnp.float32)
        carried, stacked = lax.scan(advance, (zeros, zeros), (gate_pre[layer], cells[layer, :STEPS], cells[layer, 1:], incoming), reverse=True)
        flat = stacked.reshape(STEPS * BATCH, 4 * WIDTH)
        incoming = jnp.dot(flat, w_in[layer].reshape(WIDTH, 4 * WIDTH).T, preferred_element_type=jnp.float32).reshape(STEPS, BATCH, WIDTH)
        raw_rec = jnp.dot(h_prev[layer].reshape(STEPS * BATCH, WIDTH).T, flat, preferred_element_type=jnp.float32)
        raw_in = jnp.dot(layer_in[layer].reshape(STEPS * BATCH, WIDTH).T, flat, preferred_element_type=jnp.float32)
        sumsq = sumsq + jnp.sum(raw_rec * raw_rec) + jnp.sum(raw_in * raw_in)
        rec_grads[layer] = raw_rec
        in_grads[layer] = raw_in
    scale = 1.0 / jnp.maximum(jnp.sqrt(sumsq / (8.0 * LAYERS * WIDTH * WIDTH)), 0.05)
    w_rec_grad = jnp.stack([(rec_grads[layer] * scale).reshape(WIDTH, 4, WIDTH) for layer in range(LAYERS)]).astype(jnp.bfloat16)
    w_in_grad = jnp.stack([(in_grads[layer] * scale).reshape(WIDTH, 4, WIDTH) for layer in range(LAYERS)]).astype(jnp.bfloat16)
    return (w_rec_grad, w_in_grad, incoming)
```

```python
import jax
import jax.numpy as jnp
from jax import lax
from jax.sharding import PartitionSpec as P


def cell_backward(preact, cell_prev, cell_now, hid_grad, cell_carry):
    in_gate = jax.nn.sigmoid(preact[:, 0])
    forget = jax.nn.sigmoid(preact[:, 1])
    cand_gate = jnp.tanh(preact[:, 2])
    out_gate = jax.nn.sigmoid(preact[:, 3])
    tanh_cell = jnp.tanh(cell_now)
    cell_grad = cell_carry + hid_grad * out_gate * (1.0 - tanh_cell * tanh_cell)
    grad_in = cell_grad * cand_gate * in_gate * (1.0 - in_gate)
    grad_forget = cell_grad * cell_prev * forget * (1.0 - forget)
    grad_cand = cell_grad * in_gate * (1.0 - cand_gate * cand_gate)
    grad_out = hid_grad * tanh_cell * out_gate * (1.0 - out_gate)
    gate_grads = jnp.concatenate([grad_in, grad_forget, grad_cand, grad_out], axis=1)
    return (gate_grads.astype(jnp.bfloat16), cell_grad * forget)


def contract_gates(gate_flat, weights):
    return jnp.stack(
        [
            lax.dot_general(
                gate_flat, part, (((1,), (1,)), ((), ())), preferred_element_type=jnp.float32
            )
            for part in weights
        ]
    )


def exchange(partial):
    rows = lax.axis_size("row")
    cols = lax.axis_size("col")
    ratio, count, units = partial.shape
    pieces = partial.reshape(cols, count // rows, units)
    got = lax.all_to_all(pieces, "col", 0, 0, tiled=True)
    mine = jnp.sum(got, axis=0)
    moves = [
        (r * cols + k, (k % rows) * cols + ratio * r + k // rows)
        for r in range(rows)
        for k in range(cols)
    ]
    mine = lax.ppermute(mine, ("row", "col"), moves)
    return lax.all_gather(mine, "row", axis=0, tiled=True)


def local(w_rec, w_in, gate_pre, cells, layer_in, h_prev, top_grad):
    layers, row_units, gates, col_units = w_rec.shape
    steps, batch, _ = top_grad.shape
    ratio = row_units // col_units

    def flat_parts(w):
        flat = w.reshape(layers, ratio, col_units, gates * col_units)
        return [[flat[l, i] for i in range(ratio)] for l in range(layers)]

    rec_w = flat_parts(w_rec)
    in_w = flat_parts(w_in)
    zeros = jnp.zeros((batch, col_units), jnp.float32)
    carry = [zeros] * layers
    store = [[None] * steps for _ in range(layers)]
    rec_in = [None] * layers
    for diagonal in range(steps + layers - 1):
        partials = [None] * layers
        from_above = None
        for layer in range(layers - 1, -1, -1):
            step = steps - 1 - diagonal + (layers - 1 - layer)
            if step < 0 or step >= steps:
                if from_above is not None:
                    partials[layer] = from_above
                    from_above = None
                continue
            hid = top_grad[step] if layer == layers - 1 else None
            if rec_in[layer] is not None:
                hid = rec_in[layer] if hid is None else hid + rec_in[layer]
            grads, carry[layer] = cell_backward(
                gate_pre[layer, step],
                cells[layer, step],
                cells[layer, step + 1],
                hid,
                carry[layer],
            )
            store[layer][step] = grads
            terms = []
            if step > 0:
                terms.append(contract_gates(grads, rec_w[layer]))
            if from_above is not None:
                terms.append(from_above)
            from_above = contract_gates(grads, in_w[layer]) if layer > 0 else None
            if terms:
                partials[layer] = sum(terms[1:], terms[0])
        live = [layer for layer in range(layers) if partials[layer] is not None]
        rec_in = [None] * layers
        if live:
            got = exchange(jnp.concatenate([partials[layer] for layer in live], axis=1))
            for at, layer in enumerate(live):
                rec_in[layer] = got[at * batch : (at + 1) * batch]
    flats = [jnp.concatenate(store[layer], axis=0) for layer in range(layers)]
    dx = contract_gates(flats[0], in_w[0])
    total = jnp.float32(0.0)
    for layer in range(layers):
        rec_h = h_prev[layer].reshape(steps * batch, row_units)
        in_h = layer_in[layer].reshape(steps * batch, row_units)
        nt = (((1,), (1,)), ((), ()))
        gram = lax.dot_general(flats[layer], flats[layer], nt, preferred_element_type=jnp.float32)
        gram_h = lax.dot_general(rec_h, rec_h, nt, preferred_element_type=jnp.float32)
        gram_h = gram_h + lax.dot_general(in_h, in_h, nt, preferred_element_type=jnp.float32)
        total = total + jnp.sum(gram * gram_h)
    devices = lax.axis_size("row") * lax.axis_size("col")
    spread = jnp.broadcast_to(total, (devices, 8, 128))
    spread = lax.all_to_all(spread, ("row", "col"), 0, 0, tiled=True)
    sumsq = jnp.maximum(jnp.sum(spread[:, 0, 0]), 0.0)
    input_grad = exchange(dx).reshape(steps, batch, col_units)
    width = row_units * lax.axis_size("row")
    scale = 1.0 / jnp.maximum(jnp.sqrt(sumsq / (8.0 * layers * width * width)), 0.05)

    def grads_of(saved):
        out = []
        for layer in range(layers):
            raw = lax.dot_general(
                saved[layer].reshape(steps * batch, row_units),
                flats[layer],
                (((0,), (0,)), ((), ())),
                preferred_element_type=jnp.float32,
            )
            out.append((raw * scale).astype(jnp.bfloat16).reshape(row_units, gates, col_units))
        return jnp.stack(out)

    return (grads_of(h_prev), grads_of(layer_in), input_grad)


def solution(mesh):
    placed = (
        P(None, "row", None, "col"),
        P(None, "row", None, "col"),
        P(None, None, None, None, "col"),
        P(None, None, None, "col"),
        P(None, None, None, "row"),
        P(None, None, None, "row"),
        P(None, None, "col"),
    )
    return jax.shard_map(
        local,
        mesh=mesh,
        in_specs=placed,
        out_specs=(P(None, "row", None, "col"), P(None, "row", None, "col"), P(None, None, "col")),
        check_vma=False,
    )
```

```python
import functools

import jax
import jax.numpy as jnp
from jax import lax
from jax.experimental import pallas as pl
from jax.experimental.pallas import tpu as pltpu
from jax.sharding import PartitionSpec as P

NT = (((1,), (1,)), ((), ()))
TN = (((0,), (0,)), ((), ()))
VMEM_LIMIT = 60 * 1024 * 1024
CUT = 2


def step_kernel(plan, products, *refs):
    refs = list(refs)
    live = []
    for entry in plan:
        need = ["gate", "prev", "now"] + [name for name in ("carry", "top", "got") if entry[name]]
        live.append({name: refs.pop(0) for name in need})
    weights = [[refs.pop(0) for _ in terms] for terms in products]
    for entry in plan:
        if entry["alias"]:
            refs.pop(0)
    outs = []
    for entry in plan:
        out = {"grads": refs.pop(0)}
        if entry["send"]:
            out["carry"] = refs.pop(0)
        outs.append(out)

    @pl.when(pl.program_id(0) == 0)
    def _():
        for entry, ins, out in zip(plan, live, outs):
            units = ins["prev"].shape[-1]
            gate = ins["gate"]
            in_gate = jax.nn.sigmoid(gate[0, 0, :, 0, :])
            forget = jax.nn.sigmoid(gate[0, 0, :, 1, :])
            cand_gate = jnp.tanh(gate[0, 0, :, 2, :])
            out_gate = jax.nn.sigmoid(gate[0, 0, :, 3, :])
            tanh_cell = jnp.tanh(ins["now"][0, 0])
            hid_grad = None
            if entry["top"]:
                hid_grad = ins["top"][0]
            if entry["got"]:
                batch = out["grads"].shape[0]
                got = ins["got"][pl.ds(entry["at"] * batch, batch), :]
                hid_grad = got if hid_grad is None else hid_grad + got
            cell_grad = hid_grad * out_gate * (1.0 - tanh_cell * tanh_cell)
            if entry["carry"]:
                cell_grad = cell_grad + ins["carry"][...]
            parts = (
                cell_grad * cand_gate * in_gate * (1.0 - in_gate),
                cell_grad * ins["prev"][0, 0] * forget * (1.0 - forget),
                cell_grad * in_gate * (1.0 - cand_gate * cand_gate),
                hid_grad * tanh_cell * out_gate * (1.0 - out_gate),
            )
            for k, part in enumerate(parts):
                out["grads"][:, k * units : (k + 1) * units] = part.astype(jnp.bfloat16)
            if entry["send"]:
                out["carry"][...] = cell_grad * forget

    if products:
        partial = refs.pop(0)
        for slot, (terms, w_refs) in enumerate(zip(products, weights)):
            total = None
            for which, w_ref in zip(terms, w_refs):
                grads = outs[which]["grads"]
                term = lax.dot_general(
                    grads[...], w_ref[...], NT, preferred_element_type=jnp.float32
                )
                total = term if total is None else total + term
            batch = total.shape[0]
            partial[0, slot * batch : (slot + 1) * batch, :] = total


def run_step(plan, products, gate_pre, cells, top_grad, got, carry, store):
    steps, batch, units = top_grad.shape
    tile = min(256, units)
    ins, in_specs, out_shape, out_specs, aliases = [], [], [], [], {}

    def take(array, block, index):
        ins.append(array)
        in_specs.append(pl.BlockSpec(block, lambda i: index))

    for entry in plan:
        l, t = entry["layer"], entry["step"]
        take(gate_pre, (1, 1, batch, 4, units), (l, t, 0, 0, 0))
        take(cells, (1, 1, batch, units), (l, t, 0, 0))
        take(cells, (1, 1, batch, units), (l, t + 1, 0, 0))
        if entry["carry"]:
            take(carry[l], (batch, units), (0, 0))
        if entry["top"]:
            take(top_grad, (1, batch, units), (t, 0, 0))
        if entry["got"]:
            take(got, got.shape, (0, 0))
    rows = None
    for terms in products:
        for _, weight in terms:
            rows = weight.shape[0]
            ins.append(weight)
            in_specs.append(pl.BlockSpec((tile, weight.shape[1]), lambda i: (i, 0)))
    for entry in plan:
        l, t = entry["layer"], entry["step"]
        if entry["alias"]:
            aliases[len(ins)] = len(out_shape)
            ins.append(store[l])
            in_specs.append(pl.BlockSpec(memory_space=pl.ANY))
        out_shape.append(jax.ShapeDtypeStruct((steps * batch, 4 * units), jnp.bfloat16))
        out_specs.append(pl.BlockSpec((batch, 4 * units), lambda i, t=t: (t, 0)))
        if entry["send"]:
            out_shape.append(jax.ShapeDtypeStruct((batch, units), jnp.float32))
            out_specs.append(pl.BlockSpec((batch, units), lambda i: (0, 0)))
    grid = 1
    flops = 0
    if products:
        grid = rows // tile
        per = units // tile
        count = len(products) * batch
        out_shape.append(jax.ShapeDtypeStruct((rows // units, count, units), jnp.float32))
        out_specs.append(pl.BlockSpec((1, count, tile), lambda i: (i // per, 0, i % per)))
        flops = sum(len(terms) for terms in products) * 2 * batch * rows * 4 * units
    outs = pl.pallas_call(
        functools.partial(step_kernel, plan, [[which for which, _ in terms] for terms in products]),
        grid=(grid,),
        out_shape=out_shape,
        in_specs=in_specs,
        out_specs=out_specs,
        input_output_aliases=aliases,
        compiler_params=pltpu.CompilerParams(vmem_limit_bytes=VMEM_LIMIT),
        cost_estimate=pl.CostEstimate(
            flops=flops + 1000, bytes_accessed=flops // batch + 10**6, transcendentals=0
        ),
    )(*ins)
    outs = list(outs)
    for entry in plan:
        store[entry["layer"]] = outs.pop(0)
        if entry["send"]:
            carry[entry["layer"]] = outs.pop(0)
    return outs.pop(0) if products else None


def grads_kernel(scale_ref, rec_ref, in_ref, flat_ref, rec_out, in_out, held):
    scale = scale_ref[0, 0]
    units = rec_out.shape[-1]
    for saved, out in ((rec_ref, rec_out), (in_ref, in_out)):
        for k in range(4):
            raw = lax.dot_general(
                saved[0],
                flat_ref[:, k * units : (k + 1) * units],
                TN,
                preferred_element_type=jnp.float32,
            )
            held[:, k, :] = raw * scale
        out[0] = held[...].astype(jnp.bfloat16)


def grads_kernel_keep(scale_ref, rec_ref, in_ref, flat_ref, a, b, rec_out, in_out, held):
    grads_kernel(scale_ref, rec_ref, in_ref, flat_ref, rec_out, in_out, held)


def layer_grads(layer, scale, saved_rec, saved_in, flat, before):
    layers, count, rows = saved_rec.shape
    units = flat.shape[1] // 4
    tile = min(256, rows)
    block = pl.BlockSpec((1, count, tile), lambda j: (layer, 0, j))
    kept = pl.BlockSpec(memory_space=pl.ANY)
    out = pl.BlockSpec((1, tile, 4, units), lambda j: (layer, j, 0, 0))
    return pl.pallas_call(
        grads_kernel_keep if before else grads_kernel,
        grid=(rows // tile,),
        out_shape=[jax.ShapeDtypeStruct((layers, rows, 4, units), jnp.bfloat16)] * 2,
        in_specs=[
            pl.BlockSpec(memory_space=pltpu.SMEM),
            block,
            block,
            pl.BlockSpec((count, 4 * units), lambda j: (0, 0)),
        ]
        + [kept] * len(before),
        out_specs=[out, out],
        scratch_shapes=[pltpu.VMEM((tile, 4, units), jnp.float32)],
        input_output_aliases={4: 0, 5: 1} if before else {},
        compiler_params=pltpu.CompilerParams(vmem_limit_bytes=VMEM_LIMIT),
        cost_estimate=pl.CostEstimate(
            flops=2 * 2 * count * rows * 4 * units,
            bytes_accessed=2 * rows * 4 * units * 2,
            transcendentals=0,
        ),
    )(scale, saved_rec, saved_in, flat, *before)


def swap(partial):
    cols = lax.axis_size("col")
    ratio, count, units = partial.shape
    pieces = partial.reshape(cols, ratio * count // cols, units)
    return lax.all_to_all(pieces, "col", 0, 0, tiled=True)


def place(mine):
    rows = lax.axis_size("row")
    cols = lax.axis_size("col")
    ratio = cols // rows
    moves = [
        (r * cols + k, (k % rows) * cols + ratio * r + k // rows)
        for r in range(rows)
        for k in range(cols)
    ]
    return lax.ppermute(mine, ("row", "col"), moves)


def gather(mine):
    return lax.all_gather(place(mine), "row", axis=0, tiled=True)


def gather_async(mine):
    rows = lax.axis_size("row")
    here = lax.axis_index("row")
    mine = place(mine)
    parts = [mine]
    for shift in range(1, rows):
        parts.append(lax.ppermute(mine, "row", [(i, i ^ shift) for i in range(rows)]))
    parts = jnp.stack(parts)
    return [lax.dynamic_index_in_dim(parts, here ^ i, 0, keepdims=False) for i in range(rows)]


def contract_gates(gate_flat, weight, ratio):
    parts = weight.reshape(ratio, weight.shape[0] // ratio, weight.shape[1])
    return jnp.stack(
        [
            lax.dot_general(gate_flat, parts[i], NT, preferred_element_type=jnp.float32)
            for i in range(ratio)
        ]
    )


def local(w_rec, w_in, gate_pre, cells, layer_in, h_prev, top_grad):
    layers, row_units, gates, col_units = w_rec.shape
    steps, batch, _ = top_grad.shape
    ratio = row_units // col_units
    rec_w = [w_rec[l].reshape(row_units, gates * col_units) for l in range(layers)]
    in_w = [w_in[l].reshape(row_units, gates * col_units) for l in range(layers)]
    carry = [None] * layers
    store = [None] * layers
    got = None
    bulk = None
    where = {}
    for diagonal in range(steps + layers - 1):
        plan = []
        products = {}
        for layer in range(layers - 1, -1, -1):
            step = steps - 1 - diagonal + (layers - 1 - layer)
            if step < 0 or step >= steps:
                continue
            plan.append(
                {
                    "layer": layer,
                    "step": step,
                    "carry": carry[layer] is not None,
                    "top": layer == layers - 1,
                    "got": layer in where,
                    "at": where.get(layer, 0),
                    "alias": store[layer] is not None,
                    "send": step > 0,
                }
            )
            if step > 0:
                products.setdefault(layer, []).append((len(plan) - 1, rec_w[layer]))
            if layer > 0:
                products.setdefault(layer - 1, []).append((len(plan) - 1, in_w[layer]))
        order = sorted(products, reverse=True)
        partial = run_step(
            plan, [products[l] for l in order], gate_pre, cells, top_grad, got, carry, store
        )
        if partial is not None:
            if bulk is not None:
                partial, bulk = lax.optimization_barrier((partial, bulk))
            mine = jnp.sum(swap(partial), axis=0)
            if steps - 1 - diagonal + layers - 1 == CUT:
                bulk = contract_gates(store[0][CUT * batch :], in_w[0], ratio)
                mine, bulk = lax.optimization_barrier((mine, bulk))
                bulk = swap(bulk)
            got = gather(mine)
            where = {layer: at for at, layer in enumerate(order)}
    rest = contract_gates(store[0][: CUT * batch], in_w[0], ratio)
    saved_rec = h_prev.reshape(layers, steps * batch, row_units)
    saved_in = layer_in.reshape(layers, steps * batch, row_units)
    total = jnp.float32(0.0)
    for l in range(layers):
        gram = lax.dot_general(store[l], store[l], NT, preferred_element_type=jnp.float32)
        gram_h = lax.dot_general(saved_rec[l], saved_rec[l], NT, preferred_element_type=jnp.float32)
        gram_h = gram_h + lax.dot_general(
            saved_in[l], saved_in[l], NT, preferred_element_type=jnp.float32
        )
        total = total + jnp.sum(gram * gram_h)
    devices = lax.axis_size("row") * lax.axis_size("col")
    spread = jnp.broadcast_to(total, (devices, 8, 128))
    spread = lax.all_to_all(spread, ("row", "col"), 0, 0, tiled=True)
    sumsq = jnp.maximum(jnp.sum(spread[:, 0, 0]), 0.0)
    width = row_units * lax.axis_size("row")
    scale = 1.0 / jnp.maximum(jnp.sqrt(sumsq / (8.0 * layers * width * width)), 0.05)
    scale = scale.reshape(1, 1)
    rest, scale = lax.optimization_barrier((rest, scale))
    rest = swap(rest)
    out = ()
    for l in range(layers - 1, -1, -1):
        out = tuple(layer_grads(l, scale, saved_rec, saved_in, store[l], out))
        if l == layers - 1:
            rest, *out = lax.optimization_barrier((rest, *out))
            mine = jnp.concatenate([jnp.sum(bulk, axis=0), jnp.sum(rest, axis=0)])
            parts = gather_async(mine)
    rows = lax.axis_size("row")
    count = (steps - CUT) * batch // rows
    input_grad = jnp.concatenate([p[count:] for p in parts] + [p[:count] for p in parts])
    return (out[0], out[1], input_grad.reshape(steps, batch, col_units))


def solution(mesh):
    placed = (
        P(None, "row", None, "col"),
        P(None, "row", None, "col"),
        P(None, None, None, None, "col"),
        P(None, None, None, "col"),
        P(None, None, None, "row"),
        P(None, None, None, "row"),
        P(None, None, "col"),
    )
    return jax.shard_map(
        local,
        mesh=mesh,
        in_specs=placed,
        out_specs=(P(None, "row", None, "col"), P(None, "row", None, "col"), P(None, None, "col")),
        check_vma=False,
    )
```

```python
import functools

import jax
import jax.numpy as jnp
from jax import lax
from jax.experimental import pallas as pl
from jax.experimental.pallas import tpu as pltpu
from jax.sharding import PartitionSpec as P

NT = (((1,), (1,)), ((), ()))
TN = (((0,), (0,)), ((), ()))
VMEM_LIMIT = 60 * 1024 * 1024
CUT = 2


def step_kernel(plan, products, parts, *refs):
    refs = list(refs)
    live = []
    for entry in plan:
        need = ["gate", "prev", "now"] + [name for name in ("carry", "top") if entry[name]]
        live.append({name: refs.pop(0) for name in need})
    pieces = [refs.pop(0) for _ in range(parts)]
    here = refs.pop(0) if parts else None
    weights = [[refs.pop(0) for _ in terms] for terms in products]
    for entry in plan:
        if entry["alias"]:
            refs.pop(0)
    outs = []
    for entry in plan:
        out = {"grads": refs.pop(0)}
        if entry["send"]:
            out["carry"] = refs.pop(0)
        outs.append(out)

    partial = refs.pop(0) if products else None
    whole = refs.pop(0) if parts else None

    @pl.when(pl.program_id(0) == 0)
    def _():
        for s, piece in enumerate(pieces):
            owner = lax.rem(here[0, 0] + parts - s, parts)
            size = piece.shape[0]
            whole[pl.ds(pl.multiple_of(owner * size, size), size), :] = piece[...]
        for entry, ins, out in zip(plan, live, outs):
            units = ins["prev"].shape[-1]
            gate = ins["gate"]
            in_gate = jax.nn.sigmoid(gate[0, 0, :, 0, :])
            forget = jax.nn.sigmoid(gate[0, 0, :, 1, :])
            cand_gate = jnp.tanh(gate[0, 0, :, 2, :])
            out_gate = jax.nn.sigmoid(gate[0, 0, :, 3, :])
            tanh_cell = jnp.tanh(ins["now"][0, 0])
            hid_grad = None
            if entry["top"]:
                hid_grad = ins["top"][0]
            if entry["got"]:
                batch = out["grads"].shape[0]
                got = whole[pl.ds(entry["at"] * batch, batch), :]
                hid_grad = got if hid_grad is None else hid_grad + got
            cell_grad = hid_grad * out_gate * (1.0 - tanh_cell * tanh_cell)
            if entry["carry"]:
                cell_grad = cell_grad + ins["carry"][...]
            quads = (
                cell_grad * cand_gate * in_gate * (1.0 - in_gate),
                cell_grad * ins["prev"][0, 0] * forget * (1.0 - forget),
                cell_grad * in_gate * (1.0 - cand_gate * cand_gate),
                hid_grad * tanh_cell * out_gate * (1.0 - out_gate),
            )
            for k, part in enumerate(quads):
                out["grads"][:, k * units : (k + 1) * units] = part.astype(jnp.bfloat16)
            if entry["send"]:
                out["carry"][...] = cell_grad * forget

    if products:
        for slot, (terms, w_refs) in enumerate(zip(products, weights)):
            total = None
            for which, w_ref in zip(terms, w_refs):
                grads = outs[which]["grads"]
                term = lax.dot_general(
                    grads[...], w_ref[...], NT, preferred_element_type=jnp.float32
                )
                total = term if total is None else total + term
            batch = total.shape[0]
            partial[0, slot * batch : (slot + 1) * batch, :] = total


def run_step(plan, products, gate_pre, cells, top_grad, got, carry, store):
    steps, batch, units = top_grad.shape
    tile = min(256, units)
    ins, in_specs, out_shape, out_specs, aliases = [], [], [], [], {}

    def take(array, block, index):
        ins.append(array)
        in_specs.append(pl.BlockSpec(block, lambda i: index))

    for entry in plan:
        l, t = entry["layer"], entry["step"]
        take(gate_pre, (1, 1, batch, 4, units), (l, t, 0, 0, 0))
        take(cells, (1, 1, batch, units), (l, t, 0, 0))
        take(cells, (1, 1, batch, units), (l, t + 1, 0, 0))
        if entry["carry"]:
            take(carry[l], (batch, units), (0, 0))
        if entry["top"]:
            take(top_grad, (1, batch, units), (t, 0, 0))
    scratch = []
    if got is not None:
        for piece in got:
            take(piece, piece.shape, (0, 0))
        ins.append(lax.axis_index("row").astype(jnp.int32).reshape(1, 1))
        in_specs.append(pl.BlockSpec(memory_space=pltpu.SMEM))
        scratch.append(pltpu.VMEM((len(got) * got[0].shape[0], units), jnp.float32))
    rows = None
    for terms in products:
        for _, weight in terms:
            rows = weight.shape[0]
            ins.append(weight)
            in_specs.append(pl.BlockSpec((tile, weight.shape[1]), lambda i: (i, 0)))
    for entry in plan:
        l, t = entry["layer"], entry["step"]
        if entry["alias"]:
            aliases[len(ins)] = len(out_shape)
            ins.append(store[l])
            in_specs.append(pl.BlockSpec(memory_space=pl.ANY))
        out_shape.append(jax.ShapeDtypeStruct((steps * batch, 4 * units), jnp.bfloat16))
        out_specs.append(pl.BlockSpec((batch, 4 * units), lambda i, t=t: (t, 0)))
        if entry["send"]:
            out_shape.append(jax.ShapeDtypeStruct((batch, units), jnp.float32))
            out_specs.append(pl.BlockSpec((batch, units), lambda i: (0, 0)))
    grid = 1
    flops = 0
    if products:
        grid = rows // tile
        per = units // tile
        count = len(products) * batch
        out_shape.append(jax.ShapeDtypeStruct((rows // units, count, units), jnp.float32))
        out_specs.append(pl.BlockSpec((1, count, tile), lambda i: (i // per, 0, i % per)))
        flops = sum(len(terms) for terms in products) * 2 * batch * rows * 4 * units
    outs = pl.pallas_call(
        functools.partial(
            step_kernel,
            plan,
            [[which for which, _ in terms] for terms in products],
            len(got) if got is not None else 0,
        ),
        grid=(grid,),
        out_shape=out_shape,
        in_specs=in_specs,
        out_specs=out_specs,
        scratch_shapes=scratch,
        input_output_aliases=aliases,
        compiler_params=pltpu.CompilerParams(vmem_limit_bytes=VMEM_LIMIT),
        cost_estimate=pl.CostEstimate(
            flops=flops + 1000, bytes_accessed=flops // batch + 10**6, transcendentals=0
        ),
    )(*ins)
    outs = list(outs)
    for entry in plan:
        store[entry["layer"]] = outs.pop(0)
        if entry["send"]:
            carry[entry["layer"]] = outs.pop(0)
    return outs.pop(0) if products else None


def grads_kernel(scale_ref, rec_ref, in_ref, flat_ref, rec_out, in_out, held):
    scale = scale_ref[0, 0]
    units = rec_out.shape[-1]
    for saved, out in ((rec_ref, rec_out), (in_ref, in_out)):
        for k in range(4):
            raw = lax.dot_general(
                saved[0],
                flat_ref[:, k * units : (k + 1) * units],
                TN,
                preferred_element_type=jnp.float32,
            )
            held[:, k, :] = raw * scale
        out[0] = held[...].astype(jnp.bfloat16)


def grads_kernel_keep(scale_ref, rec_ref, in_ref, flat_ref, a, b, rec_out, in_out, held):
    grads_kernel(scale_ref, rec_ref, in_ref, flat_ref, rec_out, in_out, held)


def layer_grads(layer, scale, saved_rec, saved_in, flat, before):
    layers, count, rows = saved_rec.shape
    units = flat.shape[1] // 4
    tile = min(128, rows)
    block = pl.BlockSpec((1, count, tile), lambda j: (layer, 0, j))
    kept = pl.BlockSpec(memory_space=pl.ANY)
    out = pl.BlockSpec((1, tile, 4, units), lambda j: (layer, j, 0, 0))
    return pl.pallas_call(
        grads_kernel_keep if before else grads_kernel,
        grid=(rows // tile,),
        out_shape=[jax.ShapeDtypeStruct((layers, rows, 4, units), jnp.bfloat16)] * 2,
        in_specs=[
            pl.BlockSpec(memory_space=pltpu.SMEM),
            block,
            block,
            pl.BlockSpec((count, 4 * units), lambda j: (0, 0)),
        ]
        + [kept] * len(before),
        out_specs=[out, out],
        scratch_shapes=[pltpu.VMEM((tile, 4, units), jnp.float32)],
        input_output_aliases={4: 0, 5: 1} if before else {},
        compiler_params=pltpu.CompilerParams(vmem_limit_bytes=VMEM_LIMIT),
        cost_estimate=pl.CostEstimate(
            flops=2 * 2 * count * rows * 4 * units,
            bytes_accessed=2 * rows * 4 * units * 2,
            transcendentals=0,
        ),
    )(scale, saved_rec, saved_in, flat, *before)


def swap(partial):
    cols = lax.axis_size("col")
    ratio, count, units = partial.shape
    pieces = partial.reshape(cols, ratio * count // cols, units)
    return lax.all_to_all(pieces, "col", 0, 0, tiled=True)


def place(mine):
    rows = lax.axis_size("row")
    cols = lax.axis_size("col")
    ratio = cols // rows
    moves = [
        (r * cols + k, (k % rows) * cols + ratio * r + k // rows)
        for r in range(rows)
        for k in range(cols)
    ]
    return lax.ppermute(mine, ("row", "col"), moves)


def gather(mine):
    rows = lax.axis_size("row")
    mine = place(mine)
    return [mine] + [
        lax.ppermute(mine, "row", [(i, (i + s) % rows) for i in range(rows)])
        for s in range(1, rows)
    ]


def gather_direct(mine):
    rows = lax.axis_size("row")
    cols = lax.axis_size("col")
    ratio = cols // rows
    here = lax.axis_index("row")
    parts = []
    for s in range(rows):
        moves = [
            (r * cols + k, (k + s) % rows * cols + ratio * r + k // rows)
            for r in range(rows)
            for k in range(cols)
        ]
        parts.append(lax.ppermute(mine, ("row", "col"), moves))
    parts = jnp.stack(parts)
    return [
        lax.dynamic_index_in_dim(parts, (here - i) % rows, 0, keepdims=False) for i in range(rows)
    ]


def contract_gates(gate_flat, weight, ratio):
    parts = weight.reshape(ratio, weight.shape[0] // ratio, weight.shape[1])
    return jnp.stack(
        [
            lax.dot_general(gate_flat, parts[i], NT, preferred_element_type=jnp.float32)
            for i in range(ratio)
        ]
    )


def local(w_rec, w_in, gate_pre, cells, layer_in, h_prev, top_grad):
    layers, row_units, gates, col_units = w_rec.shape
    steps, batch, _ = top_grad.shape
    ratio = row_units // col_units
    flat = (row_units, gates * col_units)
    rec_w = [None] * (layers - 1) + [w_rec[layers - 1].reshape(flat)]
    in_w = [None] * (layers - 1) + [w_in[layers - 1].reshape(flat)]
    carry = [None] * layers
    store = [None] * layers
    got = None
    bulk = None
    where = {}
    for diagonal in range(steps + layers - 1):
        plan = []
        products = {}
        for layer in range(layers - 1, -1, -1):
            step = steps - 1 - diagonal + (layers - 1 - layer)
            if step < 0 or step >= steps:
                continue
            plan.append(
                {
                    "layer": layer,
                    "step": step,
                    "carry": carry[layer] is not None,
                    "top": layer == layers - 1,
                    "got": layer in where,
                    "at": where.get(layer, 0),
                    "alias": store[layer] is not None,
                    "send": step > 0,
                }
            )
            if step > 0:
                products.setdefault(layer, []).append((len(plan) - 1, rec_w[layer]))
            if layer > 0:
                products.setdefault(layer - 1, []).append((len(plan) - 1, in_w[layer]))
        order = sorted(products, reverse=True)
        partial = run_step(
            plan, [products[l] for l in order], gate_pre, cells, top_grad, got, carry, store
        )
        if partial is not None:
            if bulk is not None:
                partial, bulk = lax.optimization_barrier((partial, bulk))
            late = rec_w if diagonal % 2 == 0 else in_w
            below = layers - 2 - diagonal // 2
            if below >= 0:
                source = w_rec if diagonal % 2 == 0 else w_in
                source, partial = lax.optimization_barrier((source, partial))
                late[below] = source[below].reshape(flat)
            partial = swap(partial)
            if below >= 0:
                partial, late[below] = lax.optimization_barrier((partial, late[below]))
            mine = jnp.sum(partial, axis=0)
            if steps - 1 - diagonal + layers - 1 == CUT:
                bulk = contract_gates(store[0][CUT * batch :], in_w[0], ratio)
                mine, bulk = lax.optimization_barrier((mine, bulk))
                bulk = swap(bulk)
            got = gather(mine)
            where = {layer: at for at, layer in enumerate(order)}
    rest = contract_gates(store[0][: CUT * batch], in_w[0], ratio)
    saved_rec = h_prev.reshape(layers, steps * batch, row_units)
    saved_in = layer_in.reshape(layers, steps * batch, row_units)
    total = jnp.float32(0.0)
    for l in range(layers):
        gram = lax.dot_general(store[l], store[l], NT, preferred_element_type=jnp.float32)
        gram_h = lax.dot_general(saved_rec[l], saved_rec[l], NT, preferred_element_type=jnp.float32)
        gram_h = gram_h + lax.dot_general(
            saved_in[l], saved_in[l], NT, preferred_element_type=jnp.float32
        )
        total = total + jnp.sum(gram * gram_h)
    devices = lax.axis_size("row") * lax.axis_size("col")
    spread = jnp.broadcast_to(total, (devices, 8, 128))
    spread = lax.all_to_all(spread, ("row", "col"), 0, 0, tiled=True)
    sumsq = jnp.maximum(jnp.sum(spread[:, 0, 0]), 0.0)
    width = row_units * lax.axis_size("row")
    scale = 1.0 / jnp.maximum(jnp.sqrt(sumsq / (8.0 * layers * width * width)), 0.05)
    scale = scale.reshape(1, 1)
    rest, scale = lax.optimization_barrier((rest, scale))
    rest = swap(rest)
    out = ()
    for l in range(layers - 1, -1, -1):
        out = tuple(layer_grads(l, scale, saved_rec, saved_in, store[l], out))
        if l == layers - 1:
            rest, *out = lax.optimization_barrier((rest, *out))
            mine = jnp.concatenate([jnp.sum(bulk, axis=0), jnp.sum(rest, axis=0)])
            parts = gather_direct(mine)
    rows = lax.axis_size("row")
    count = (steps - CUT) * batch // rows
    input_grad = jnp.concatenate([p[count:] for p in parts] + [p[:count] for p in parts])
    return (out[0], out[1], input_grad.reshape(steps, batch, col_units))


def solution(mesh):
    placed = (
        P(None, "row", None, "col"),
        P(None, "row", None, "col"),
        P(None, None, None, None, "col"),
        P(None, None, None, "col"),
        P(None, None, None, "row"),
        P(None, None, None, "row"),
        P(None, None, "col"),
    )
    return jax.shard_map(
        local,
        mesh=mesh,
        in_specs=placed,
        out_specs=(P(None, "row", None, "col"), P(None, "row", None, "col"), P(None, None, "col")),
        check_vma=False,
    )
```

```python
import functools

import jax
import jax.numpy as jnp
from jax import lax
from jax.experimental import pallas as pl
from jax.experimental.pallas import tpu as pltpu
from jax.sharding import PartitionSpec as P

NT = (((1,), (1,)), ((), ()))
TN = (((0,), (0,)), ((), ()))
VMEM_LIMIT = 60 * 1024 * 1024
CUT = 2


def step_kernel(plan, products, parts, *refs):
    refs = list(refs)
    live = []
    for entry in plan:
        need = ["gate", "prev", "now"] + [name for name in ("carry", "top") if entry[name]]
        live.append({name: refs.pop(0) for name in need})
    pieces = [refs.pop(0) for _ in range(parts)]
    here = refs.pop(0) if parts else None
    weights = [[refs.pop(0) for _ in terms] for terms in products]
    for entry in plan:
        if entry["alias"]:
            refs.pop(0)
    outs = []
    for entry in plan:
        out = {"grads": refs.pop(0)}
        if entry["send"]:
            out["carry"] = refs.pop(0)
        outs.append(out)

    partial = refs.pop(0) if products else None
    whole = refs.pop(0) if parts else None

    @pl.when(pl.program_id(0) == 0)
    def _():
        for s, piece in enumerate(pieces):
            owner = lax.rem(here[0, 0] + parts - s, parts)
            size = piece.shape[0]
            whole[pl.ds(pl.multiple_of(owner * size, size), size), :] = piece[...]
        for entry, ins, out in zip(plan, live, outs):
            units = ins["prev"].shape[-1]
            gate = ins["gate"]
            in_gate = jax.nn.sigmoid(gate[0, 0, :, 0, :])
            forget = jax.nn.sigmoid(gate[0, 0, :, 1, :])
            cand_gate = jnp.tanh(gate[0, 0, :, 2, :])
            out_gate = jax.nn.sigmoid(gate[0, 0, :, 3, :])
            tanh_cell = jnp.tanh(ins["now"][0, 0])
            hid_grad = None
            if entry["top"]:
                hid_grad = ins["top"][0]
            if entry["got"]:
                batch = out["grads"].shape[0]
                got = whole[pl.ds(entry["at"] * batch, batch), :]
                hid_grad = got if hid_grad is None else hid_grad + got
            cell_grad = hid_grad * out_gate * (1.0 - tanh_cell * tanh_cell)
            if entry["carry"]:
                cell_grad = cell_grad + ins["carry"][...]
            quads = (
                cell_grad * cand_gate * in_gate * (1.0 - in_gate),
                cell_grad * ins["prev"][0, 0] * forget * (1.0 - forget),
                cell_grad * in_gate * (1.0 - cand_gate * cand_gate),
                hid_grad * tanh_cell * out_gate * (1.0 - out_gate),
            )
            for k, part in enumerate(quads):
                out["grads"][:, k * units : (k + 1) * units] = part.astype(jnp.bfloat16)
            if entry["send"]:
                out["carry"][...] = cell_grad * forget

    if products:
        for slot, (terms, w_refs) in enumerate(zip(products, weights)):
            total = None
            for which, w_ref in zip(terms, w_refs):
                grads = outs[which]["grads"]
                term = lax.dot_general(
                    grads[...], w_ref[...], NT, preferred_element_type=jnp.float32
                )
                total = term if total is None else total + term
            batch = total.shape[0]
            partial[0, slot * batch : (slot + 1) * batch, :] = total


def run_step(plan, products, gate_pre, cells, top_grad, got, carry, store):
    steps, batch, units = top_grad.shape
    tile = min(256, units)
    ins, in_specs, out_shape, out_specs, aliases = [], [], [], [], {}

    def take(array, block, index):
        ins.append(array)
        in_specs.append(pl.BlockSpec(block, lambda i: index))

    for entry in plan:
        l, t = entry["layer"], entry["step"]
        take(gate_pre, (1, 1, batch, 4, units), (l, t, 0, 0, 0))
        take(cells, (1, 1, batch, units), (l, t, 0, 0))
        take(cells, (1, 1, batch, units), (l, t + 1, 0, 0))
        if entry["carry"]:
            take(carry[l], (batch, units), (0, 0))
        if entry["top"]:
            take(top_grad, (1, batch, units), (t, 0, 0))
    scratch = []
    if got is not None:
        for piece in got:
            take(piece, piece.shape, (0, 0))
        ins.append(lax.axis_index("row").astype(jnp.int32).reshape(1, 1))
        in_specs.append(pl.BlockSpec(memory_space=pltpu.SMEM))
        scratch.append(pltpu.VMEM((len(got) * got[0].shape[0], units), jnp.float32))
    rows = None
    for terms in products:
        for _, weight in terms:
            rows = weight.shape[0]
            ins.append(weight)
            in_specs.append(pl.BlockSpec((tile, weight.shape[1]), lambda i: (i, 0)))
    for entry in plan:
        l, t = entry["layer"], entry["step"]
        if entry["alias"]:
            aliases[len(ins)] = len(out_shape)
            ins.append(store[l])
            in_specs.append(pl.BlockSpec(memory_space=pl.ANY))
        out_shape.append(jax.ShapeDtypeStruct((steps * batch, 4 * units), jnp.bfloat16))
        out_specs.append(pl.BlockSpec((batch, 4 * units), lambda i, t=t: (t, 0)))
        if entry["send"]:
            out_shape.append(jax.ShapeDtypeStruct((batch, units), jnp.float32))
            out_specs.append(pl.BlockSpec((batch, units), lambda i: (0, 0)))
    grid = 1
    flops = 0
    if products:
        grid = rows // tile
        per = units // tile
        count = len(products) * batch
        out_shape.append(jax.ShapeDtypeStruct((rows // units, count, units), jnp.float32))
        out_specs.append(pl.BlockSpec((1, count, tile), lambda i: (i // per, 0, i % per)))
        flops = sum(len(terms) for terms in products) * 2 * batch * rows * 4 * units
    outs = pl.pallas_call(
        functools.partial(
            step_kernel,
            plan,
            [[which for which, _ in terms] for terms in products],
            len(got) if got is not None else 0,
        ),
        grid=(grid,),
        out_shape=out_shape,
        in_specs=in_specs,
        out_specs=out_specs,
        scratch_shapes=scratch,
        input_output_aliases=aliases,
        compiler_params=pltpu.CompilerParams(vmem_limit_bytes=VMEM_LIMIT),
        cost_estimate=pl.CostEstimate(
            flops=flops + 1000, bytes_accessed=flops // batch + 10**6, transcendentals=0
        ),
    )(*ins)
    outs = list(outs)
    for entry in plan:
        store[entry["layer"]] = outs.pop(0)
        if entry["send"]:
            carry[entry["layer"]] = outs.pop(0)
    return outs.pop(0) if products else None


def grads_kernel(scale_ref, rec_ref, in_ref, flat_ref, rec_out, in_out, held):
    scale = scale_ref[0, 0]
    units = rec_out.shape[-1]
    for saved, out in ((rec_ref, rec_out), (in_ref, in_out)):
        for k in range(4):
            raw = lax.dot_general(
                saved[0],
                flat_ref[:, k * units : (k + 1) * units],
                TN,
                preferred_element_type=jnp.float32,
            )
            held[:, k, :] = raw * scale
        out[0] = held[...].astype(jnp.bfloat16)


def grads_kernel_keep(scale_ref, rec_ref, in_ref, flat_ref, a, b, rec_out, in_out, held):
    grads_kernel(scale_ref, rec_ref, in_ref, flat_ref, rec_out, in_out, held)


def layer_grads(layer, scale, saved_rec, saved_in, flat, before):
    layers, count, rows = saved_rec.shape
    units = flat.shape[1] // 4
    tile = min(128, rows)
    block = pl.BlockSpec((1, count, tile), lambda j: (layer, 0, j))
    kept = pl.BlockSpec(memory_space=pl.ANY)
    out = pl.BlockSpec((1, tile, 4, units), lambda j: (layer, j, 0, 0))
    return pl.pallas_call(
        grads_kernel_keep if before else grads_kernel,
        grid=(rows // tile,),
        out_shape=[jax.ShapeDtypeStruct((layers, rows, 4, units), jnp.bfloat16)] * 2,
        in_specs=[
            pl.BlockSpec(memory_space=pltpu.SMEM),
            block,
            block,
            pl.BlockSpec((count, 4 * units), lambda j: (0, 0)),
        ]
        + [kept] * len(before),
        out_specs=[out, out],
        scratch_shapes=[pltpu.VMEM((tile, 4, units), jnp.float32)],
        input_output_aliases={4: 0, 5: 1} if before else {},
        compiler_params=pltpu.CompilerParams(vmem_limit_bytes=VMEM_LIMIT),
        cost_estimate=pl.CostEstimate(
            flops=2 * 2 * count * rows * 4 * units,
            bytes_accessed=2 * rows * 4 * units * 2,
            transcendentals=0,
        ),
    )(scale, saved_rec, saved_in, flat, *before)


def swap(partial):
    cols = lax.axis_size("col")
    ratio, count, units = partial.shape
    pieces = partial.reshape(cols, ratio * count // cols, units)
    return lax.all_to_all(pieces, "col", 0, 0, tiled=True)


def place(mine):
    rows = lax.axis_size("row")
    cols = lax.axis_size("col")
    ratio = cols // rows
    moves = [
        (r * cols + k, (k % rows) * cols + ratio * r + k // rows)
        for r in range(rows)
        for k in range(cols)
    ]
    return lax.ppermute(mine, ("row", "col"), moves)


def gather(mine):
    rows = lax.axis_size("row")
    mine = place(mine)
    return [mine] + [
        lax.ppermute(mine, "row", [(i, (i + s) % rows) for i in range(rows)])
        for s in range(1, rows)
    ]


def gather_ordered(mine):
    rows = lax.axis_size("row")
    here = lax.axis_index("row")
    parts = jnp.stack(gather(mine))
    return [
        lax.dynamic_index_in_dim(parts, (here - i) % rows, 0, keepdims=False) for i in range(rows)
    ]


def contract_gates(gate_flat, weight, ratio):
    parts = weight.reshape(ratio, weight.shape[0] // ratio, weight.shape[1])
    return jnp.stack(
        [
            lax.dot_general(gate_flat, parts[i], NT, preferred_element_type=jnp.float32)
            for i in range(ratio)
        ]
    )


def local(w_rec, w_in, gate_pre, cells, layer_in, h_prev, top_grad):
    layers, row_units, gates, col_units = w_rec.shape
    steps, batch, _ = top_grad.shape
    ratio = row_units // col_units
    flat = (row_units, gates * col_units)
    rec_w = [None] * (layers - 1) + [w_rec[layers - 1].reshape(flat)]
    in_w = [None] * (layers - 1) + [w_in[layers - 1].reshape(flat)]
    carry = [None] * layers
    store = [None] * layers
    got = None
    bulk = None
    where = {}
    for diagonal in range(steps + layers - 1):
        plan = []
        products = {}
        for layer in range(layers - 1, -1, -1):
            step = steps - 1 - diagonal + (layers - 1 - layer)
            if step < 0 or step >= steps:
                continue
            plan.append(
                {
                    "layer": layer,
                    "step": step,
                    "carry": carry[layer] is not None,
                    "top": layer == layers - 1,
                    "got": layer in where,
                    "at": where.get(layer, 0),
                    "alias": store[layer] is not None,
                    "send": step > 0,
                }
            )
            if step > 0:
                products.setdefault(layer, []).append((len(plan) - 1, rec_w[layer]))
            if layer > 0:
                products.setdefault(layer - 1, []).append((len(plan) - 1, in_w[layer]))
        order = sorted(products, reverse=True)
        partial = run_step(
            plan, [products[l] for l in order], gate_pre, cells, top_grad, got, carry, store
        )
        if partial is not None:
            if bulk is not None:
                partial, bulk = lax.optimization_barrier((partial, bulk))
            late = rec_w if diagonal % 2 == 0 else in_w
            below = layers - 2 - diagonal // 2
            if below >= 0:
                source = w_rec if diagonal % 2 == 0 else w_in
                source, partial = lax.optimization_barrier((source, partial))
                late[below] = source[below].reshape(flat)
            partial = swap(partial)
            if below >= 0:
                partial, late[below] = lax.optimization_barrier((partial, late[below]))
            mine = jnp.sum(partial, axis=0)
            if steps - 1 - diagonal + layers - 1 == CUT:
                bulk = contract_gates(store[0][CUT * batch :], in_w[0], ratio)
                mine, bulk = lax.optimization_barrier((mine, bulk))
                bulk = swap(bulk)
            got = gather(mine)
            where = {layer: at for at, layer in enumerate(order)}
    rest = contract_gates(store[0][: CUT * batch], in_w[0], ratio)
    saved_rec = h_prev.reshape(layers, steps * batch, row_units)
    saved_in = layer_in.reshape(layers, steps * batch, row_units)
    total = jnp.float32(0.0)
    for l in range(layers):
        gram = lax.dot_general(store[l], store[l], NT, preferred_element_type=jnp.float32)
        gram_h = lax.dot_general(saved_rec[l], saved_rec[l], NT, preferred_element_type=jnp.float32)
        gram_h = gram_h + lax.dot_general(
            saved_in[l], saved_in[l], NT, preferred_element_type=jnp.float32
        )
        total = total + jnp.sum(gram * gram_h)
    devices = lax.axis_size("row") * lax.axis_size("col")
    spread = jnp.broadcast_to(total, (devices, 8, 128))
    spread = lax.all_to_all(spread, ("row", "col"), 0, 0, tiled=True)
    sumsq = jnp.maximum(jnp.sum(spread[:, 0, 0]), 0.0)
    width = row_units * lax.axis_size("row")
    scale = 1.0 / jnp.maximum(jnp.sqrt(sumsq / (8.0 * layers * width * width)), 0.05)
    scale = scale.reshape(1, 1)
    rest, scale = lax.optimization_barrier((rest, scale))
    rest = swap(rest)
    out = ()
    for l in range(layers - 1, -1, -1):
        out = tuple(layer_grads(l, scale, saved_rec, saved_in, store[l], out))
        if l == layers - 1:
            rest, *out = lax.optimization_barrier((rest, *out))
            mine = jnp.concatenate([jnp.sum(bulk, axis=0), jnp.sum(rest, axis=0)])
            parts = gather_ordered(mine)
    rows = lax.axis_size("row")
    count = (steps - CUT) * batch // rows
    input_grad = jnp.concatenate([p[count:] for p in parts] + [p[:count] for p in parts])
    return (out[0], out[1], input_grad.reshape(steps, batch, col_units))


def solution(mesh):
    placed = (
        P(None, "row", None, "col"),
        P(None, "row", None, "col"),
        P(None, None, None, None, "col"),
        P(None, None, None, "col"),
        P(None, None, None, "row"),
        P(None, None, None, "row"),
        P(None, None, "col"),
    )
    return jax.shard_map(
        local,
        mesh=mesh,
        in_specs=placed,
        out_specs=(P(None, "row", None, "col"), P(None, "row", None, "col"), P(None, None, "col")),
        check_vma=False,
    )
```

```python
import functools

import jax
import jax.numpy as jnp
from jax import lax
from jax.experimental import pallas as pl
from jax.experimental.pallas import tpu as pltpu
from jax.sharding import PartitionSpec as P

NT = (((1,), (1,)), ((), ()))
TN = (((0,), (0,)), ((), ()))
VMEM_LIMIT = 60 * 1024 * 1024
CUT = 3


def step_kernel(plan, products, parts, *refs):
    refs = list(refs)
    live = []
    for entry in plan:
        need = ["gate", "prev", "now"] + [name for name in ("carry", "top") if entry[name]]
        live.append({name: refs.pop(0) for name in need})
    pieces = [refs.pop(0) for _ in range(parts)]
    here = refs.pop(0) if parts else None
    weights = [[refs.pop(0) for _ in terms] for terms in products]
    for entry in plan:
        if entry["alias"]:
            refs.pop(0)
    outs = []
    for entry in plan:
        out = {"grads": refs.pop(0)}
        if entry["send"]:
            out["carry"] = refs.pop(0)
        outs.append(out)

    partial = refs.pop(0) if products else None
    whole = refs.pop(0) if parts else None

    @pl.when(pl.program_id(0) == 0)
    def _():
        for s, piece in enumerate(pieces):
            owner = lax.rem(here[0, 0] + parts - s, parts)
            size = piece.shape[0]
            whole[pl.ds(pl.multiple_of(owner * size, size), size), :] = piece[...]
        for entry, ins, out in zip(plan, live, outs):
            units = ins["prev"].shape[-1]
            gate = ins["gate"]
            in_gate = jax.nn.sigmoid(gate[0, 0, :, 0, :])
            forget = jax.nn.sigmoid(gate[0, 0, :, 1, :])
            cand_gate = jnp.tanh(gate[0, 0, :, 2, :])
            out_gate = jax.nn.sigmoid(gate[0, 0, :, 3, :])
            tanh_cell = jnp.tanh(ins["now"][0, 0])
            hid_grad = None
            if entry["top"]:
                hid_grad = ins["top"][0]
            if entry["got"]:
                batch = out["grads"].shape[0]
                got = whole[pl.ds(entry["at"] * batch, batch), :]
                hid_grad = got if hid_grad is None else hid_grad + got
            cell_grad = hid_grad * out_gate * (1.0 - tanh_cell * tanh_cell)
            if entry["carry"]:
                cell_grad = cell_grad + ins["carry"][...]
            quads = (
                cell_grad * cand_gate * in_gate * (1.0 - in_gate),
                cell_grad * ins["prev"][0, 0] * forget * (1.0 - forget),
                cell_grad * in_gate * (1.0 - cand_gate * cand_gate),
                hid_grad * tanh_cell * out_gate * (1.0 - out_gate),
            )
            for k, part in enumerate(quads):
                out["grads"][:, k * units : (k + 1) * units] = part.astype(jnp.bfloat16)
            if entry["send"]:
                out["carry"][...] = cell_grad * forget

    if products:
        for slot, (terms, w_refs) in enumerate(zip(products, weights)):
            total = None
            for which, w_ref in zip(terms, w_refs):
                grads = outs[which]["grads"]
                term = lax.dot_general(
                    grads[...], w_ref[...], NT, preferred_element_type=jnp.float32
                )
                total = term if total is None else total + term
            batch = total.shape[0]
            partial[0, slot * batch : (slot + 1) * batch, :] = total


def run_step(plan, products, gate_pre, cells, top_grad, got, carry, store):
    steps, batch, units = top_grad.shape
    tile = min(256, units)
    ins, in_specs, out_shape, out_specs, aliases = [], [], [], [], {}

    def take(array, block, index):
        ins.append(array)
        in_specs.append(pl.BlockSpec(block, lambda i: index))

    for entry in plan:
        l, t = entry["layer"], entry["step"]
        take(gate_pre, (1, 1, batch, 4, units), (l, t, 0, 0, 0))
        take(cells, (1, 1, batch, units), (l, t, 0, 0))
        take(cells, (1, 1, batch, units), (l, t + 1, 0, 0))
        if entry["carry"]:
            take(carry[l], (batch, units), (0, 0))
        if entry["top"]:
            take(top_grad, (1, batch, units), (t, 0, 0))
    scratch = []
    if got is not None:
        for piece in got:
            take(piece, piece.shape, (0, 0))
        ins.append(lax.axis_index("row").astype(jnp.int32).reshape(1, 1))
        in_specs.append(pl.BlockSpec(memory_space=pltpu.SMEM))
        scratch.append(pltpu.VMEM((len(got) * got[0].shape[0], units), jnp.float32))
    rows = None
    for terms in products:
        for _, weight in terms:
            rows = weight.shape[0]
            ins.append(weight)
            in_specs.append(pl.BlockSpec((tile, weight.shape[1]), lambda i: (i, 0)))
    for entry in plan:
        l, t = entry["layer"], entry["step"]
        if entry["alias"]:
            aliases[len(ins)] = len(out_shape)
            ins.append(store[l])
            in_specs.append(pl.BlockSpec(memory_space=pl.ANY))
        out_shape.append(jax.ShapeDtypeStruct((steps * batch, 4 * units), jnp.bfloat16))
        out_specs.append(pl.BlockSpec((batch, 4 * units), lambda i, t=t: (t, 0)))
        if entry["send"]:
            out_shape.append(jax.ShapeDtypeStruct((batch, units), jnp.float32))
            out_specs.append(pl.BlockSpec((batch, units), lambda i: (0, 0)))
    grid = 1
    flops = 0
    if products:
        grid = rows // tile
        per = units // tile
        count = len(products) * batch
        out_shape.append(jax.ShapeDtypeStruct((rows // units, count, units), jnp.float32))
        out_specs.append(pl.BlockSpec((1, count, tile), lambda i: (i // per, 0, i % per)))
        flops = sum(len(terms) for terms in products) * 2 * batch * rows * 4 * units
    outs = pl.pallas_call(
        functools.partial(
            step_kernel,
            plan,
            [[which for which, _ in terms] for terms in products],
            len(got) if got is not None else 0,
        ),
        grid=(grid,),
        out_shape=out_shape,
        in_specs=in_specs,
        out_specs=out_specs,
        scratch_shapes=scratch,
        input_output_aliases=aliases,
        compiler_params=pltpu.CompilerParams(vmem_limit_bytes=VMEM_LIMIT),
        cost_estimate=pl.CostEstimate(
            flops=flops + 1000, bytes_accessed=flops // batch + 10**6, transcendentals=0
        ),
    )(*ins)
    outs = list(outs)
    for entry in plan:
        store[entry["layer"]] = outs.pop(0)
        if entry["send"]:
            carry[entry["layer"]] = outs.pop(0)
    return outs.pop(0) if products else None


def grads_kernel(scale_ref, rec_ref, in_ref, flat_ref, rec_out, in_out, held):
    scale = scale_ref[0, 0]
    units = rec_out.shape[-1]
    for saved, out in ((rec_ref, rec_out), (in_ref, in_out)):
        for k in range(4):
            raw = lax.dot_general(
                saved[0],
                flat_ref[:, k * units : (k + 1) * units],
                TN,
                preferred_element_type=jnp.float32,
            )
            held[:, k, :] = raw * scale
        out[0] = held[...].astype(jnp.bfloat16)


def grads_kernel_keep(scale_ref, rec_ref, in_ref, flat_ref, a, b, rec_out, in_out, held):
    grads_kernel(scale_ref, rec_ref, in_ref, flat_ref, rec_out, in_out, held)


def layer_grads(layer, scale, saved_rec, saved_in, flat, before):
    layers, count, rows = saved_rec.shape
    units = flat.shape[1] // 4
    tile = min(128, rows)
    block = pl.BlockSpec((1, count, tile), lambda j: (layer, 0, j))
    kept = pl.BlockSpec(memory_space=pl.ANY)
    out = pl.BlockSpec((1, tile, 4, units), lambda j: (layer, j, 0, 0))
    return pl.pallas_call(
        grads_kernel_keep if before else grads_kernel,
        grid=(rows // tile,),
        out_shape=[jax.ShapeDtypeStruct((layers, rows, 4, units), jnp.bfloat16)] * 2,
        in_specs=[
            pl.BlockSpec(memory_space=pltpu.SMEM),
            block,
            block,
            pl.BlockSpec((count, 4 * units), lambda j: (0, 0)),
        ]
        + [kept] * len(before),
        out_specs=[out, out],
        scratch_shapes=[pltpu.VMEM((tile, 4, units), jnp.float32)],
        input_output_aliases={4: 0, 5: 1} if before else {},
        compiler_params=pltpu.CompilerParams(vmem_limit_bytes=VMEM_LIMIT),
        cost_estimate=pl.CostEstimate(
            flops=2 * 2 * count * rows * 4 * units,
            bytes_accessed=2 * rows * 4 * units * 2,
            transcendentals=0,
        ),
    )(scale, saved_rec, saved_in, flat, *before)


def swap(partial):
    cols = lax.axis_size("col")
    ratio, count, units = partial.shape
    pieces = partial.reshape(cols, ratio * count // cols, units)
    return lax.all_to_all(pieces, "col", 0, 0, tiled=True)


def place(mine):
    rows = lax.axis_size("row")
    cols = lax.axis_size("col")
    ratio = cols // rows
    moves = [
        (r * cols + k, (k % rows) * cols + ratio * r + k // rows)
        for r in range(rows)
        for k in range(cols)
    ]
    return lax.ppermute(mine, ("row", "col"), moves)


def gather(mine):
    rows = lax.axis_size("row")
    mine = place(mine)
    return [mine] + [
        lax.ppermute(mine, "row", [(i, (i + s) % rows) for i in range(rows)])
        for s in range(1, rows)
    ]


def gather_ordered(mine):
    rows = lax.axis_size("row")
    here = lax.axis_index("row")
    parts = jnp.stack(gather(mine))
    return [
        lax.dynamic_index_in_dim(parts, (here - i) % rows, 0, keepdims=False) for i in range(rows)
    ]


def contract_gates(gate_flat, weight, ratio):
    parts = weight.reshape(ratio, weight.shape[0] // ratio, weight.shape[1])
    return jnp.stack(
        [
            lax.dot_general(gate_flat, parts[i], NT, preferred_element_type=jnp.float32)
            for i in range(ratio)
        ]
    )


def local(w_rec, w_in, gate_pre, cells, layer_in, h_prev, top_grad):
    layers, row_units, gates, col_units = w_rec.shape
    steps, batch, _ = top_grad.shape
    ratio = row_units // col_units
    flat = (row_units, gates * col_units)
    rec_w = [None] * (layers - 1) + [w_rec[layers - 1].reshape(flat)]
    in_w = [None] * (layers - 1) + [w_in[layers - 1].reshape(flat)]
    carry = [None] * layers
    store = [None] * layers
    got = None
    bulk = None
    where = {}
    for diagonal in range(steps + layers - 1):
        plan = []
        products = {}
        for layer in range(layers - 1, -1, -1):
            step = steps - 1 - diagonal + (layers - 1 - layer)
            if step < 0 or step >= steps:
                continue
            plan.append(
                {
                    "layer": layer,
                    "step": step,
                    "carry": carry[layer] is not None,
                    "top": layer == layers - 1,
                    "got": layer in where,
                    "at": where.get(layer, 0),
                    "alias": store[layer] is not None,
                    "send": step > 0,
                }
            )
            if step > 0:
                products.setdefault(layer, []).append((len(plan) - 1, rec_w[layer]))
            if layer > 0:
                products.setdefault(layer - 1, []).append((len(plan) - 1, in_w[layer]))
        order = sorted(products, reverse=True)
        partial = run_step(
            plan, [products[l] for l in order], gate_pre, cells, top_grad, got, carry, store
        )
        if partial is not None:
            if bulk is not None:
                partial, bulk = lax.optimization_barrier((partial, bulk))
            late = rec_w if diagonal % 2 == 0 else in_w
            below = layers - 2 - diagonal // 2
            if below >= 0:
                source = w_rec if diagonal % 2 == 0 else w_in
                source, partial = lax.optimization_barrier((source, partial))
                late[below] = source[below].reshape(flat)
            partial = swap(partial)
            if below >= 0:
                partial, late[below] = lax.optimization_barrier((partial, late[below]))
            mine = jnp.sum(partial, axis=0)
            if steps - 1 - diagonal + layers - 1 == CUT:
                bulk = contract_gates(store[0][CUT * batch :], in_w[0], ratio)
                mine, bulk = lax.optimization_barrier((mine, bulk))
                bulk = swap(bulk)
            got = gather(mine)
            where = {layer: at for at, layer in enumerate(order)}
    rest = contract_gates(store[0][: CUT * batch], in_w[0], ratio)
    saved_rec = h_prev.reshape(layers, steps * batch, row_units)
    saved_in = layer_in.reshape(layers, steps * batch, row_units)
    total = jnp.float32(0.0)
    for l in range(layers):
        gram = lax.dot_general(store[l], store[l], NT, preferred_element_type=jnp.float32)
        gram_h = lax.dot_general(saved_rec[l], saved_rec[l], NT, preferred_element_type=jnp.float32)
        gram_h = gram_h + lax.dot_general(
            saved_in[l], saved_in[l], NT, preferred_element_type=jnp.float32
        )
        total = total + jnp.sum(gram * gram_h)
    devices = lax.axis_size("row") * lax.axis_size("col")
    spread = jnp.broadcast_to(total, (devices, 8, 128))
    spread = lax.all_to_all(spread, ("row", "col"), 0, 0, tiled=True)
    sumsq = jnp.maximum(jnp.sum(spread[:, 0, 0]), 0.0)
    width = row_units * lax.axis_size("row")
    scale = 1.0 / jnp.maximum(jnp.sqrt(sumsq / (8.0 * layers * width * width)), 0.05)
    scale = scale.reshape(1, 1)
    rest, scale = lax.optimization_barrier((rest, scale))
    rest = swap(rest)
    out = ()
    for l in range(layers - 1, -1, -1):
        out = tuple(layer_grads(l, scale, saved_rec, saved_in, store[l], out))
        if l == layers - 1:
            rest, *out = lax.optimization_barrier((rest, *out))
            mine = jnp.concatenate([jnp.sum(bulk, axis=0), jnp.sum(rest, axis=0)])
            parts = gather_ordered(mine)
    rows = lax.axis_size("row")
    count = (steps - CUT) * batch // rows
    input_grad = jnp.concatenate([p[count:] for p in parts] + [p[:count] for p in parts])
    return (out[0], out[1], input_grad.reshape(steps, batch, col_units))


def solution(mesh):
    placed = (
        P(None, "row", None, "col"),
        P(None, "row", None, "col"),
        P(None, None, None, None, "col"),
        P(None, None, None, "col"),
        P(None, None, None, "row"),
        P(None, None, None, "row"),
        P(None, None, "col"),
    )
    return jax.shard_map(
        local,
        mesh=mesh,
        in_specs=placed,
        out_specs=(P(None, "row", None, "col"), P(None, "row", None, "col"), P(None, None, "col")),
        check_vma=False,
    )
```
